32 devices in a mesh: wide: 8 (over y, x, core), narrow: 4 (over z).
Axes of the slice: x: 2, y: 2, z: 4, core: 2. Of those that a mesh axis runs over, the one named last changes fastest.
Arguments:
- expression: bfloat16 [4000, 49152], P(None, ('wide', 'narrow')), may hold values from -60 to 60
- sketch_map: bfloat16 [64, 4000], replicated, may hold values from -0.09375 to 0.09375
Outputs:
- projected: float32 [64, 4000], P(None, 'narrow')
The draws below stay inside these ranges and needn't reach their ends.
All inputs are finite; a program needn't handle non-finite values.
Results may differ from the reference program's by a relative error of at most 0.00037.
Values sent between devices are 32-bit elements; how exact they have to be, the bound alone decides.
A program may use at most 64 MiB of HBM per device.

```python
import jax
import jax.numpy as jnp
from jax import lax

GENES = 4000
SKETCH = 64
CELLS = 49152


def draw_expression(key, part):
    first, second, third = jax.random.split(jax.random.fold_in(key, 17), 3)
    position = jnp.arange(CELLS, dtype=jnp.float32) / CELLS
    cell_scale = jnp.exp(jnp.log(10.0) * (0.5 * position + 0.5 * jax.random.uniform(second, (CELLS,), jnp.float32)))
    base = jnp.clip(jax.random.normal(first, (GENES, CELLS), jnp.float32), -6.0, 6.0)
    gene_scale = 0.5 + jax.random.uniform(third, (GENES,), jnp.float32)
    values = base * gene_scale[:, None] * cell_scale[None, :]
    return jnp.clip(values, -60.0, 60.0).astype(jnp.bfloat16)


def gaussian(own_key, extent, scale, most, kind=jnp.bfloat16):
    return jnp.clip(scale * jax.random.normal(own_key, extent, jnp.float32), -most, most).astype(kind)


def setup_inputs(seed: int = 0) -> dict:
    key_of = jax.random.split(jax.random.key(seed), 3)
    expression = draw_expression(jax.random.fold_in(key_of[2], 71), 0)
    sketch_map = gaussian(key_of[1], (SKETCH, GENES), GENES ** -0.5, 0.09375)
    return dict(expression=expression, sketch_map=sketch_map)


def reference(expression, sketch_map):
    sketched = jnp.dot(sketch_map.astype(jnp.float32), expression.astype(jnp.float32), preferred_element_type=jnp.float32).astype(jnp.bfloat16)
    gram = lax.dot_general(sketched.astype(jnp.float32), sketched.astype(jnp.float32), (((1,), (1,)), ((), ())), preferred_element_type=jnp.float32)
    lower = jnp.linalg.cholesky(gram)
    products = lax.dot_general(sketched.astype(jnp.float32), expression.astype(jnp.float32), (((1,), (1,)), ((), ())), preferred_element_type=jnp.float32)
    projected = lax.linalg.triangular_solve(lower, products, left_side=True, lower=True)
    return projected
```

```python
import functools

import jax
import jax.numpy as jnp
from jax import lax
from jax.experimental import pallas as pl
from jax.experimental.pallas import tpu as pltpu
from jax.sharding import PartitionSpec as P

LANES = 128
SUBLANES = 8
DEPTH = 512
PIECES = 4
LAG = 1
GRAM_AT = 1
EARLY = 40


def window_of(z, genes_own, width, padded):
    start = (z * genes_own) // LANES * LANES
    return jnp.minimum(start, padded - width)


def eliminate(blocks, first, last):
    row_id = lax.broadcasted_iota(jnp.int32, (SUBLANES, 1), 0)
    blocks = list(blocks)
    for k in range(first, last):
        home, r = divmod(k, SUBLANES)
        row = blocks[home][r : r + 1, :]
        scaled = row / row[:, k : k + 1]
        for i in range(home, len(blocks)):
            factor = blocks[i][:, k : k + 1]
            if i == home:
                factor = jnp.where(row_id > r, factor, 0.0)
            blocks[i] = blocks[i] - factor * scaled
    return blocks


def kernel(
    nw, nn, genes_own, width, padded, halvings,
    e_hbm, s_hbm, out_ref,
    e_ref, s_ref, skf, sk_ref, acc, gram, gat, zrecv, grecv, gzrecv, *rest,
):
    stages = max(nw.bit_length() - 1, 1)
    recvs = rest[:stages]
    (load_sem, st_send, st_recv, z_send, z_recv, ga_send, ga_recv, gr_send, gr_recv, gz_send, gz_recv) = rest[stages:]
    sketch, genes = s_ref.shape
    cells = e_ref.shape[1]
    w = lax.axis_index("wide")
    z = lax.axis_index("narrow")
    core = w % 2

    loads = [pltpu.make_async_copy(s_hbm, s_ref, load_sem.at[0])]
    cuts = list(range(0, genes, DEPTH)) + [genes]
    for b in range(len(cuts) - 1):
        rows = pl.ds(cuts[b], cuts[b + 1] - cuts[b])
        loads.append(pltpu.make_async_copy(e_hbm.at[rows], e_ref.at[rows], load_sem.at[b + 1]))
    for load in loads:
        load.start()

    def flip(power):
        return w + power - 2 * power * ((w // power) % 2)

    later = list(range(1, stages))
    turn = len(later) // 2
    other = later[turn:] + later[:turn]
    powers = [1] + [2**a + core * (2**b - 2**a) for a, b in zip(later, other)]
    peers = []
    for mask in range(1, 2 ** (halvings - 1)):
        peer = w
        for t in range(1, halvings):
            if mask >> (t - 1) & 1:
                peer = peer + powers[t] - 2 * powers[t] * ((w // powers[t]) % 2)
        peers.append((mask, peer))
    diagonal = [peer for mask, peer in peers if mask & (mask - 1)]

    barrier = pltpu.get_barrier_semaphore()
    for peer in diagonal:
        pl.semaphore_signal(barrier, inc=1, device_id={"wide": peer, "narrow": z})
    for t in range(stages):
        pl.semaphore_signal(barrier, inc=1, device_id={"wide": flip(2**t), "narrow": z})
    for d in range(1, nn):
        pl.semaphore_signal(barrier, inc=1, device_id={"wide": w, "narrow": (z + d) % nn})

    loads[0].wait()
    for b in range(len(cuts) - 1):
        loads[b + 1].wait()
        span = slice(cuts[b], cuts[b + 1])
        part = jnp.dot(s_ref[:, span], e_ref[span, :], preferred_element_type=jnp.float32)
        skf[...] = part if b == 0 else skf[...] + part
    sk = skf[...].astype(jnp.bfloat16)
    sk_ref[...] = sk
    total = lax.dot_general(sk, sk, (((1,), (1,)), ((), ())), preferred_element_type=jnp.float32)
    gram[...] = jnp.zeros_like(gram)
    gram[:, :sketch] = total
    pl.semaphore_wait(barrier, stages + nn - 1 + len(diagonal))

    bases, sizes = [], []
    base, size = 0, sketch
    for t in range(stages):
        if t < halvings:
            size //= 2
            bit = (w // powers[t]) % 2
            bases.append((pl.multiple_of(base + size * bit, SUBLANES), pl.multiple_of(base + size * (1 - bit), SUBLANES)))
            base = bases[-1][0]
        else:
            bases.append((base, base))
        sizes.append(size)

    def gram_copy(t):
        return pltpu.make_async_remote_copy(
            src_ref=gram, dst_ref=grecv.at[t], send_sem=gr_send.at[t], recv_sem=gr_recv.at[t],
            device_id={"wide": flip(2**t), "narrow": z},
        )

    def gram_z_copies():
        return [
            pltpu.make_async_remote_copy(
                src_ref=gram, dst_ref=gzrecv.at[d - 1], send_sem=gz_send.at[d - 1], recv_sem=gz_recv.at[d - 1],
                device_id={"wide": w, "narrow": (z + d) % nn},
            )
            for d in range(1, nn)
        ]

    chain = []

    def gram_next():
        t = len(chain)
        if t > stages:
            return
        if t > 0:
            chain[-1].wait()
            gram[...] = gram[...] + grecv[t - 1]
        if t < stages:
            copy = gram_copy(t)
            copy.start()
            chain.append(copy)
        else:
            copies = gram_z_copies()
            for copy in copies:
                copy.start()
            chain.append(copies)

    piece = padded // PIECES

    def stage_copy(t, p):
        lanes = pl.ds(p * piece, piece)
        return pltpu.make_async_remote_copy(
            src_ref=acc.at[pl.ds(bases[t][1], sizes[t]), lanes],
            dst_ref=recvs[t].at[:, lanes],
            send_sem=st_send.at[t, p], recv_sem=st_recv.at[t, p],
            device_id={"wide": flip(powers[t]), "narrow": z},
        )

    flying = {}

    def stage_start(t, p):
        flying[t, p] = stage_copy(t, p)
        flying[t, p].start()

    def stage_end(t, p):
        flying[t, p].wait()
        lanes = pl.ds(p * piece, piece)
        rows = pl.ds(bases[t][0], sizes[t])
        acc[rows, lanes] = acc[rows, lanes] + recvs[t][:, lanes]

    gram_next()
    if padded > genes:
        edge = genes // LANES * LANES
        acc[:, edge:] = jnp.zeros((sketch, padded - edge), jnp.float32)
    for p in range(PIECES):
        stop = min((p + 1) * piece, genes)
        acc[:, p * piece : stop] = lax.dot_general(
            sk_ref[...], e_ref[p * piece : stop, :], (((1,), (1,)), ((), ())),
            preferred_element_type=jnp.float32,
        )
        stage_start(0, p)
        if p == 1:
            gram_next()
        if p >= LAG:
            stage_end(0, p - LAG)
            if stages > 1:
                stage_start(1, p - LAG)
    gram_next()
    for p in range(PIECES - LAG, PIECES):
        stage_end(0, p)
        if stages > 1:
            stage_start(1, p)
    for t in range(1, stages):
        for p in range(PIECES):
            stage_end(t, p)
            if t + 1 < stages:
                stage_start(t + 1, p)
            if p == GRAM_AT:
                gram_next()

    own_rows = pl.ds(bases[-1][0], sizes[-1])
    z_copies = []
    for d in range(1, nn):
        to = (z + d) % nn
        start = pl.multiple_of(window_of(to, genes_own, width, padded), LANES)
        z_copies.append(
            pltpu.make_async_remote_copy(
                src_ref=acc.at[own_rows, pl.ds(start, width)], dst_ref=zrecv.at[d - 1],
                send_sem=z_send.at[d - 1], recv_sem=z_recv.at[d - 1],
                device_id={"wide": w, "narrow": to},
            )
        )
        z_copies[-1].start()
    while len(chain) <= stages:
        gram_next()
    for copy in chain[-1]:
        copy.wait()
    whole = gram[...]
    for d in range(1, nn):
        whole = whole + gzrecv[d - 1]
    lane = lax.broadcasted_iota(jnp.int32, (sketch, LANES), 1)
    line = lax.broadcasted_iota(jnp.int32, (sketch, LANES), 0)
    whole = jnp.where(lane == line + sketch, 1.0, whole)
    blocks = [whole[i : i + SUBLANES] for i in range(0, sketch, SUBLANES)]
    done = EARLY
    blocks = eliminate(blocks, 0, done)
    start = pl.multiple_of(window_of(z, genes_own, width, padded), LANES)
    mine = acc[own_rows, pl.ds(start, width)]
    for d in range(1, nn):
        z_copies[d - 1].wait()
        mine = mine + zrecv[d - 1]
    gat[own_rows, :] = mine
    def gather(rows, i, peer):
        return pltpu.make_async_remote_copy(
            src_ref=gat.at[rows], dst_ref=gat.at[rows],
            send_sem=ga_send.at[i], recv_sem=ga_recv.at[i],
            device_id={"wide": peer, "narrow": z},
        )

    copies = [gather(own_rows, mask, peer) for mask, peer in reversed(peers)]
    for copy in copies:
        copy.start()
    blocks = eliminate(blocks, done, sketch)
    reduced = jnp.concatenate(blocks, axis=0)
    pivots = jnp.sum(jnp.where(lane == line, reduced, 0.0), axis=1, keepdims=True)
    inverse = (reduced / jnp.sqrt(pivots))[:, sketch:]
    for copy in copies:
        copy.wait()
    copy = gather(pl.ds(bases[0][0], sizes[0]), 0, flip(1))
    copy.start()
    copy.wait()
    result = jnp.dot(
        inverse, gat[...], preferred_element_type=jnp.float32, precision=lax.Precision.HIGHEST
    )
    shift = z * genes_own - window_of(z, genes_own, width, padded)
    out_ref[...] = pltpu.roll(result, (width - shift) % width, 1)[:, :genes_own]


def solution(mesh):
    nw, nn = mesh.shape["wide"], mesh.shape["narrow"]

    def on_device(expression, sketch_map):
        genes, cells = expression.shape
        sketch = sketch_map.shape[0]
        genes_own = genes // nn
        padded = -(-genes // (LANES * PIECES)) * LANES * PIECES
        width = max(
            -(-(i + 1) * genes_own // LANES) - i * genes_own // LANES for i in range(nn)
        ) * LANES
        stages = nw.bit_length() - 1
        halvings = min(stages, (sketch // SUBLANES).bit_length() - 1)
        sizes = [max(sketch >> (t + 1), sketch >> halvings) for t in range(stages)]
        last = sizes[-1]
        dma = pltpu.SemaphoreType.DMA
        return pl.pallas_call(
            functools.partial(kernel, nw, nn, genes_own, width, padded, halvings),
            out_shape=pltpu.VMEM((sketch, genes_own), jnp.float32),
            in_specs=[pl.BlockSpec(memory_space=pl.ANY)] * 2,
            out_specs=pl.BlockSpec(memory_space=pltpu.VMEM),
            scratch_shapes=[
                pltpu.VMEM((genes, cells), jnp.bfloat16),
                pltpu.VMEM((sketch, genes), jnp.bfloat16),
                pltpu.VMEM((sketch, cells), jnp.float32),
                pltpu.VMEM((sketch, cells), jnp.bfloat16),
                pltpu.VMEM((sketch, padded), jnp.float32),
                pltpu.VMEM((sketch, LANES), jnp.float32),
                pltpu.VMEM((sketch, width), jnp.float32),
                pltpu.VMEM((nn - 1, last, width), jnp.float32),
                pltpu.VMEM((stages, sketch, LANES), jnp.float32),
                pltpu.VMEM((nn - 1, sketch, LANES), jnp.float32),
            ]
            + [pltpu.VMEM((size, padded), jnp.float32) for size in sizes]
            + [
                dma((-(-genes // DEPTH) + 1,)),
                dma((stages, PIECES)),
                dma((stages, PIECES)),
                dma((nn - 1,)),
                dma((nn - 1,)),
                dma((2 ** (halvings - 1),)),
                dma((2 ** (halvings - 1),)),
                dma((stages,)),
                dma((stages,)),
                dma((nn - 1,)),
                dma((nn - 1,)),
            ],
            compiler_params=pltpu.CompilerParams(collective_id=0, has_side_effects=True),
        )(expression, sketch_map)

    placed = (P(None, ("wide", "narrow")), P())
    return jax.shard_map(
        on_device, mesh=mesh, in_specs=placed, out_specs=P(None, "narrow"), check_vma=False
    )
```
